32 devices in a mesh: batch: 8 (over z, y), rows: 4 (over x, core).
Axes of the slice: x: 2, y: 2, z: 4, core: 2. Of those that a mesh axis runs over, the one named last changes fastest.
Arguments:
- features: bfloat16 [192, 14, 14, 1024], P(('batch', 'rows')), may hold values from -12 to 12
- grads: bfloat16 [192, 14, 14, 256], P(('batch', 'rows')), may hold values from -12 to 12
- kernel: bfloat16 [3, 3, 256, 1024], replicated, may hold values from -0.125 to 0.125
- vectors: float32 [16, 64, 64], replicated, may hold values from -1 to 1, as said below
- values: float32 [16, 64], replicated, may hold values from 0.05 to 2
Outputs:
- input_grad: bfloat16 [192, 14, 14, 1024], P(('batch', 'rows'))
- kernel_grad: float32 [1024, 3, 3, 256], P(('batch', 'rows'))
The draws below stay inside these ranges and needn't reach their ends.
Inputs may be any that keep to these rules, and one draw needn't show every extreme that they name: `vectors`: each group's matrix is orthogonal.
All inputs are finite; a program needn't handle non-finite values.
Results may differ from the reference program's by a relative error of at most 0.015.
Values sent between devices are 32-bit elements; how exact they have to be, the bound alone decides.
A program may use at most 128 MiB of HBM per device.

```python
import math
import jax
import jax.numpy as jnp
from jax import lax

D = 1024
GSIZE = 64
COUT = 256
WD = 14
HEIGHT = 14
IMG_DEV = 6
GROUPS = 16
IMAGES = 192
DEVICES = 32


def draw_features(key, part):
    key_offset, key_spread, key_noise = jax.random.split(jax.random.fold_in(key, 11), 3)
    offsets = 0.5 * jax.random.normal(key_offset, (D,), jnp.float32)
    spread = jnp.exp(jax.random.uniform(key_spread, (D,), jnp.float32, math.log(0.5), math.log(2.0)))
    ramp = 1.0 + 2.0 * jnp.arange(IMAGES, dtype=jnp.float32) / max(IMAGES - 1, 1)
    noise = jax.random.normal(key_noise, (IMAGES, HEIGHT, WD, D), jnp.float32)
    result = offsets * ramp[:, None, None, None] + spread * noise
    return jnp.clip(result, -12.0, 12.0).astype(jnp.bfloat16)


def draw_grads(key, part):
    key_offset, key_spread, key_noise = jax.random.split(jax.random.fold_in(key, 23), 3)
    offsets = 0.3 * jax.random.normal(key_offset, (COUT,), jnp.float32)
    spread = jnp.exp(jax.random.uniform(key_spread, (COUT,), jnp.float32, math.log(0.5), math.log(2.0)))
    ramp = 1.0 + 2.0 * jnp.arange(IMAGES, dtype=jnp.float32) / max(IMAGES - 1, 1)
    noise = jax.random.normal(key_noise, (IMAGES, HEIGHT, WD, COUT), jnp.float32)
    result = offsets * ramp[:, None, None, None] + spread * noise
    return jnp.clip(result, -12.0, 12.0).astype(jnp.bfloat16)


def draw_vectors(key, part):
    matrices = jax.random.normal(jax.random.fold_in(key, 37), (GROUPS, GSIZE, GSIZE), jnp.float32)
    basis, unused = jnp.linalg.qr(matrices)
    return basis.astype(jnp.float32)


def normal_values(rng, shape, deviation, most, kind=jnp.bfloat16):
    return jnp.clip(deviation * jax.random.normal(rng, shape, jnp.float32), -most, most).astype(kind)


def setup_inputs(seed: int = 0) -> dict:
    keys = jax.random.split(jax.random.key(seed), 6)
    features = draw_features(jax.random.fold_in(keys[5], 71), 0)
    grads = draw_grads(jax.random.fold_in(keys[5], 71), 0)
    kernel = normal_values(keys[2], (3, 3, COUT, D), (9 * COUT) ** -0.5, 0.125)
    vectors = draw_vectors(jax.random.fold_in(keys[5], 71), 0)
    values = jnp.clip(jnp.exp(jax.random.uniform(keys[4], (GROUPS, GSIZE), jnp.float32, math.log(0.05), math.log(2.0))), 0.05, 2.0)
    return {"features": features, "grads": grads, "kernel": kernel, "vectors": vectors, "values": values}


highest = lax.Precision.HIGHEST

def whitening(vectors, values):
    scales = lax.rsqrt(values)
    whiten = jnp.einsum('gij,gj,gkj->gik', vectors, scales, vectors, precision=highest)
    return (scales, whiten)

def block_matrix(blocks):
    groups, group_size = (blocks.shape[0], blocks.shape[1])
    identity = jnp.eye(groups, dtype=jnp.float32)
    full = jnp.einsum('gh,gij->gihj', identity, blocks, precision=highest)
    return full.reshape(groups * group_size, groups * group_size)

def diagonal_blocks(full, groups, group_size):
    shaped = full.reshape(groups, group_size, groups, group_size)
    index = jnp.arange(groups)
    return shaped[index, :, index, :]

def gather_columns(padded, slab_rows, columns_count):
    outputs = padded.shape[3]
    pieces = [padded[:, 2 - shift_row:2 - shift_row + slab_rows, 2 - shift_col:2 - shift_col + columns_count, :] for shift_row in range(3) for shift_col in range(3)]
    return jnp.concatenate(pieces, axis=3).reshape(-1, 9 * outputs)

def reference(features, grads, kernel, vectors, values):
    group_size = values.shape[1]
    groups = values.shape[0]
    channels = features.shape[3]
    outputs = grads.shape[3]
    pixel_total = 1.0 * features.shape[0] * features.shape[1] * features.shape[2]
    feature_blocks = features.reshape(DEVICES, IMG_DEV, HEIGHT, WD, channels)
    grad_blocks = grads.reshape(DEVICES, IMG_DEV, HEIGHT, WD, outputs)
    kernel_flat = kernel.reshape(9 * outputs, channels)
    scales, whiten = whitening(vectors, values)
    whiten_low = block_matrix(whiten).astype(jnp.bfloat16)

    def add_sums(carry, block):
        return (carry + lax.optimization_barrier(jnp.sum(block.reshape(-1, channels), axis=0, dtype=jnp.float32)), None)
    sum_feature, unused = lax.scan(add_sums, jnp.zeros((channels,), jnp.float32), feature_blocks)
    channel_mean = sum_feature / pixel_total

    def block_terms(feature_block, grad_block):
        flat = feature_block.reshape(-1, channels)
        centered_low = (flat.astype(jnp.float32) - channel_mean).astype(jnp.bfloat16)
        padded = jnp.pad(grad_block, ((0, 0), (1, 1), (1, 1), (0, 0)))
        columns = gather_columns(padded, HEIGHT, WD)
        back_grad = jnp.dot(columns.astype(jnp.float32), kernel_flat.astype(jnp.float32), preferred_element_type=jnp.float32)
        return (flat, centered_low, columns, back_grad)

    def accumulate(carry, blocks):
        cov_part, back_part, weight_part = carry
        flat, centered_low, columns, back_grad = block_terms(blocks[0], blocks[1])
        whitened = jnp.dot(centered_low.astype(jnp.float32), whiten_low.astype(jnp.float32), preferred_element_type=jnp.float32).astype(jnp.bfloat16)
        back_low = back_grad.astype(jnp.bfloat16)
        cov_part = cov_part + lax.dot_general(flat.astype(jnp.float32), back_low.astype(jnp.float32), (((0,), (0,)), ((), ())), preferred_element_type=jnp.float32)
        back_part = back_part + lax.optimization_barrier(jnp.sum(back_grad, axis=0))
        weight_part = weight_part + lax.dot_general(whitened.astype(jnp.float32), columns.astype(jnp.float32), (((0,), (0,)), ((), ())), preferred_element_type=jnp.float32)
        return ((cov_part, back_part, weight_part), None)
    start_carry = (jnp.zeros((channels, channels), jnp.float32), jnp.zeros((channels,), jnp.float32), jnp.zeros((channels, 9 * outputs), jnp.float32))
    totals, unused = lax.scan(accumulate, start_carry, (feature_blocks, grad_blocks))
    raw_full, back_total, weight_total = totals
    raw_cov = diagonal_blocks(raw_full, groups, group_size)
    cov_grad = raw_cov - channel_mean.reshape(groups, group_size)[:, :, None] * back_total.reshape(groups, group_size)[:, None, :]
    rotated = jnp.einsum('gki,gkl,glj->gij', vectors, cov_grad, vectors, precision=highest)
    symmetric = 0.5 * (rotated + jnp.swapaxes(rotated, 1, 2))
    roots = jnp.sqrt(values)
    factor = -(scales[:, :, None] * scales[:, None, :]) / (roots[:, :, None] + roots[:, None, :])
    sigma_grad = jnp.einsum('gik,gkl,gjl->gij', vectors, symmetric * factor, vectors, precision=highest)
    sigma_low = block_matrix(2.0 / pixel_total * sigma_grad).astype(jnp.bfloat16)
    stacked = jnp.concatenate([whiten_low, sigma_low], axis=0)

    def input_block(blocks):
        flat, centered_low, columns, back_grad = block_terms(blocks[0], blocks[1])
        shifted_low = (back_grad - back_total / pixel_total).astype(jnp.bfloat16)
        joined = jnp.concatenate([shifted_low, centered_low], axis=1)
        result = jnp.dot(joined.astype(jnp.float32), stacked.astype(jnp.float32), preferred_element_type=jnp.float32)
        return result.reshape(IMG_DEV, HEIGHT, WD, channels).astype(jnp.bfloat16)
    input_grad = lax.map(input_block, (feature_blocks, grad_blocks)).reshape(features.shape)
    kernel_grad = weight_total.reshape(channels, 3, 3, outputs)
    return (input_grad, kernel_grad)
```

```python
import functools
import jax
import jax.numpy as jnp
from jax import lax
from jax.experimental import pallas as pl
from jax.experimental.pallas import tpu as pltpu
from jax.sharding import PartitionSpec as P

highest = lax.Precision.HIGHEST
F32, BF16 = jnp.float32, jnp.bfloat16
LANES = 128
VMEM_LIMIT = 60 * 1024 * 1024


def round_up(n, m):
    return (n + m - 1) // m * m


def bit_orders(bits):
    rest = list(range(1, bits))
    first = [0] + rest
    second = [0] + rest[1:2] + rest[:1] + rest[2:]
    third = [0] + rest[2:3] + rest[:2] + rest[3:]
    return [first, second, third]


def slot_of(index, order):
    slot = 0
    count = len(order)
    for step, bit in enumerate(order):
        slot = slot + (index // 2**bit) % 2 * 2 ** (count - 1 - step)
    return slot


def products_kernel(
    sizes, f_ref, g_ref, k_ref, w_ref, pieces_ref, back_ref, small_ref, fp, cols, gpad
):
    images, height, width, wide, channels, outputs, per, orders = sizes
    rows = images * height * wide
    kp = fp.shape[0]
    blocks = channels // LANES
    taps = 3 * outputs

    fp[pl.ds(rows, kp - rows), :] = jnp.zeros((kp - rows, channels), BF16)
    cols[pl.ds(rows, kp - rows), :] = jnp.zeros((kp - rows, 3 * taps), BF16)
    gpad[...] = jnp.zeros(gpad.shape, F32)

    @pl.loop(0, images)
    def _(b):
        gpad[pl.ds(1, height), pl.ds(1, width), :] = g_ref[b].astype(F32)
        for h in range(height):
            at = pl.multiple_of((b * height + h) * wide, 16)
            fp[pl.ds(at, wide), :] = jnp.zeros((wide, channels), BF16)
            fp[pl.ds(at, width), :] = f_ref[b, h]
        for c in range(3):
            shifted = gpad[:, 2 - c : 2 - c + wide, :].astype(BF16)
            for a in range(3):
                at = pl.multiple_of(b * height * wide, 16)
                cols[pl.ds(at, height * wide), a * taps + c * outputs : a * taps + (c + 1) * outputs] = (
                    shifted[2 - a : 2 - a + height].reshape(height * wide, outputs)
                )

    position = lax.broadcasted_iota(jnp.int32, (kp, 1), 0)
    valid = (position % wide < width) & (position < rows)
    lane = lax.broadcasted_iota(jnp.int32, (8, kp), 1)
    ones = jnp.where((lane % wide < width) & (lane < rows), 1.0, 0.0).astype(BF16)
    half = LANES // 2
    low_lane = lax.broadcasted_iota(jnp.int32, (half, LANES), 1) < half
    base = channels // 2
    small_ref[pl.ds(base, small_ref.shape[0] - base), :] = jnp.zeros(
        (small_ref.shape[0] - base, LANES), F32
    )

    step = 2 * LANES

    @pl.loop(0, channels // step)
    def _(n):
        at = pl.ds(pl.multiple_of(n * step, step), step)
        back = jnp.dot(cols[...], k_ref[:, at], preferred_element_type=F32)
        back_ref[:, at] = back
        total = jnp.sum(jnp.where(valid, back, 0.0), axis=0, keepdims=True)
        low = back.astype(BF16)
        feature = fp[:, at]
        raw = lax.dot_general(
            feature, low, (((0,), (0,)), ((), ())), preferred_element_type=F32
        )
        fsum = jnp.dot(ones, feature, preferred_element_type=F32)
        for q in range(2):
            block = raw[q * LANES : (q + 1) * LANES, q * LANES : (q + 1) * LANES]
            where = pl.multiple_of((2 * n + q) * half, half)
            small_ref[pl.ds(where, half), :] = jnp.where(low_lane, block[:half], block[half:])
            small_ref[pl.ds(base + 2 * n + q, 1), :] = total[:, q * LANES : (q + 1) * LANES]
            small_ref[pl.ds(base + blocks + 2 * n + q, 1), :] = fsum[
                :1, q * LANES : (q + 1) * LANES
            ]

    colsum = jnp.dot(ones, cols[...], preferred_element_type=F32)
    for q in range(3 * taps // LANES):
        small_ref[pl.ds(base + 2 * blocks + q, 1), :] = colsum[:1, q * LANES : (q + 1) * LANES]

    @pl.loop(0, blocks)
    def _(k):
        feature = fp[:, pl.ds(pl.multiple_of(k * LANES, LANES), LANES)]
        weight = w_ref[k]
        for a in range(3):
            part = lax.dot_general(
                feature,
                cols[:, a * taps : (a + 1) * taps],
                (((0,), (0,)), ((), ())),
                preferred_element_type=F32,
            )
            one = part.astype(BF16)
            left = part - one.astype(F32)
            two = left.astype(BF16)
            three = (left - two.astype(F32)).astype(BF16)
            result = (
                jnp.dot(weight, one, preferred_element_type=F32)
                + jnp.dot(weight, two, preferred_element_type=F32)
                + jnp.dot(weight, three, preferred_element_type=F32)
            )
            for j in range(LANES // per):
                slot = slot_of(k * (LANES // per) + j, orders[a])
                pieces_ref[a, slot] = result[j * per : (j + 1) * per]


def comm_kernel(shape, orders, pieces_ref, small_ref, share_ref, total_ref, *scratch):
    nb, nr = shape
    bits = len(orders[0])
    count = 2**bits
    streams = len(orders)
    recv = [[scratch[s * bits + t] for t in range(bits)] for s in range(streams)]
    small_recv = scratch[streams * bits : streams * bits + bits]
    send_sem, recv_sem = scratch[-2:]
    batch = lax.axis_index("batch")
    row = lax.axis_index("rows")
    index = batch * nr + row

    def bit_of(bit):
        return (index // 2**bit) % 2

    def partner(bit):
        sign = 1 - 2 * bit_of(bit)
        if 2**bit < nr:
            return (batch, row + sign * 2**bit)
        return (batch + sign * (2**bit // nr), row)

    barrier = pltpu.get_barrier_semaphore()
    for bit in range(bits):
        pl.semaphore_signal(
            barrier, inc=1, device_id=partner(bit), device_id_type=pl.DeviceIdType.MESH
        )
    pl.semaphore_wait(barrier, bits)

    def copy(src, dst, s, t, bit):
        return pltpu.make_async_remote_copy(
            src_ref=src,
            dst_ref=dst,
            send_sem=send_sem.at[s, t],
            recv_sem=recv_sem.at[s, t],
            device_id=partner(bit),
            device_id_type=pl.DeviceIdType.MESH,
        )

    sources = [pieces_ref.at[a] for a in range(streams)] + [small_ref]
    buffers = recv + [list(small_recv)]
    all_orders = list(orders) + [orders[0]]
    sequence = [streams] + list(range(streams))

    def begin(s, t):
        bit = all_orders[s][t]
        size = count >> (t + 1)
        src = sources[s] if t == 0 else buffers[s][t - 1]
        c = copy(src.at[pl.ds((1 - bit_of(bit)) * size, size)], buffers[s][t], s, t, bit)
        c.start()
        return c

    def finish(s, t, c):
        bit = all_orders[s][t]
        size = count >> (t + 1)
        src = sources[s] if t == 0 else buffers[s][t - 1]
        dst = buffers[s][t]
        c.wait()
        first = bit_of(bit) * size

        @pl.loop(0, size)
        def _(i):
            dst[i] = dst[i] + src[first + i]

    flights = {s: begin(s, 0) for s in sequence}
    for t in range(bits):
        for s in sequence:
            finish(s, t, flights[s])
            if t + 1 < bits:
                flights[s] = begin(s, t + 1)
            elif s < streams:
                share_ref[s] = buffers[s][t][0]
            else:
                slot = slot_of(index, all_orders[s])
                total_ref[slot] = buffers[s][t][0]
                for u in range(bits):
                    bit = all_orders[s][bits - 1 - u]
                    region = pl.ds(slot // 2**u * 2**u, 2**u)
                    c = copy(total_ref.at[region], total_ref.at[region], s, bits + u, bit)
                    c.start()
                    c.wait()


def final_kernel(height, width, wide, b_ref, f_ref, w_ref, s_ref, bt_ref, m_ref, o_ref, cent):
    channels = f_ref.shape[3]
    for h in range(height):
        cent[pl.ds(h * wide, width), :] = (f_ref[0, h].astype(F32) - m_ref[...]).astype(BF16)
    for k in range(channels // LANES):
        at = slice(k * LANES, (k + 1) * LANES)
        shifted = (b_ref[:, at] - bt_ref[:, at]).astype(BF16)
        out = jnp.dot(shifted, w_ref[k], preferred_element_type=F32) + jnp.dot(
            cent[:, at], s_ref[k], preferred_element_type=F32
        )
        out = out.astype(BF16).reshape(height, wide, LANES)
        o_ref[0, :, :, at] = out[:, :width]


def pair_blocks(blocks):
    groups, size = blocks.shape[:2]
    pairs = blocks.reshape(groups // 2, 2, size, size)
    zero = jnp.zeros((groups // 2, size, size), blocks.dtype)
    top = jnp.concatenate([pairs[:, 0], zero], axis=2)
    bottom = jnp.concatenate([zero, pairs[:, 1]], axis=2)
    return jnp.concatenate([top, bottom], axis=1)


def local(shape, features, grads, kernel, vectors, values):
    images, height, width, channels = features.shape
    outputs = grads.shape[3]
    groups, group_size = values.shape
    devices = shape[0] * shape[1]
    bits = devices.bit_length() - 1
    orders = bit_orders(bits)
    per = channels // devices
    taps = 3 * outputs
    wide = round_up(width, 16)
    rows = images * height * wide
    kp = round_up(rows + 1, LANES)
    blocks = channels // LANES
    pixel_total = 1.0 * images * height * width * devices
    small_rows = channels // 2 + 2 * blocks + 3 * taps // LANES
    rp = round_up(-(-small_rows // devices), 8)

    scales = lax.rsqrt(values)
    whiten = jnp.einsum("gij,gj,gkj->gik", vectors, scales, vectors, precision=highest)
    w_pairs = pair_blocks(whiten.astype(BF16))
    vmem = pl.BlockSpec(memory_space=pltpu.VMEM)

    sizes = (images, height, width, wide, channels, outputs, per, orders)
    pieces, back, small = pl.pallas_call(
        functools.partial(products_kernel, sizes),
        out_shape=(
            jax.ShapeDtypeStruct((3, devices, per, taps), F32),
            jax.ShapeDtypeStruct((kp, channels), F32),
            jax.ShapeDtypeStruct((devices * rp, LANES), F32),
        ),
        in_specs=[vmem] * 4,
        out_specs=(vmem,) * 3,
        scratch_shapes=[
            pltpu.VMEM((kp, channels), BF16),
            pltpu.VMEM((kp, 3 * taps), BF16),
            pltpu.VMEM((height + 2, wide + 8, outputs), F32),
        ],
        compiler_params=pltpu.CompilerParams(vmem_limit_bytes=VMEM_LIMIT),
        name="products",
    )(features, grads, kernel.reshape(3 * taps, channels), jnp.swapaxes(w_pairs, 1, 2))

    scratch = []
    for _ in range(3):
        scratch += [pltpu.VMEM((devices >> (t + 1), per, taps), F32) for t in range(bits)]
    scratch += [pltpu.VMEM((devices >> (t + 1), rp, LANES), F32) for t in range(bits)]
    scratch += [pltpu.SemaphoreType.DMA((4, 2 * bits))] * 2
    share, total = pl.pallas_call(
        functools.partial(comm_kernel, shape, orders),
        out_shape=(
            jax.ShapeDtypeStruct((3, per, taps), F32),
            jax.ShapeDtypeStruct((devices, rp, LANES), F32),
        ),
        in_specs=[vmem] * 2,
        out_specs=(vmem,) * 2,
        scratch_shapes=scratch,
        compiler_params=pltpu.CompilerParams(
            collective_id=0, has_side_effects=True, vmem_limit_bytes=VMEM_LIMIT
        ),
        name="exchange",
    )(pieces, small.reshape(devices, rp, LANES))

    total = total.reshape(devices * rp, LANES)
    base = channels // 2
    raw_cov = (
        total[:base]
        .reshape(groups // 2, group_size, 2, group_size)
        .transpose(0, 2, 1, 3)
        .reshape(groups, group_size, group_size)
    )
    back_total = total[base : base + blocks].reshape(channels)
    channel_mean = total[base + blocks : base + 2 * blocks].reshape(channels) / pixel_total
    colsum = total[base + 2 * blocks : small_rows].reshape(3, taps)

    cov_grad = (
        raw_cov
        - channel_mean.reshape(groups, group_size)[:, :, None]
        * back_total.reshape(groups, group_size)[:, None, :]
    )
    rotated = jnp.einsum("gki,gkl,glj->gij", vectors, cov_grad, vectors, precision=highest)
    symmetric = 0.5 * (rotated + jnp.swapaxes(rotated, 1, 2))
    roots = jnp.sqrt(values)
    factor = -(scales[:, :, None] * scales[:, None, :]) / (roots[:, :, None] + roots[:, None, :])
    sigma_grad = jnp.einsum(
        "gik,gkl,gjl->gij", vectors, symmetric * factor, vectors, precision=highest
    )
    s_pairs = pair_blocks((2.0 / pixel_total * sigma_grad).astype(BF16))

    image_rows = height * wide
    whole = lambda *dims: pl.BlockSpec(dims, lambda i: (0,) * len(dims))
    input_grad = pl.pallas_call(
        functools.partial(final_kernel, height, width, wide),
        grid=(images,),
        out_shape=jax.ShapeDtypeStruct(features.shape, BF16),
        in_specs=[
            pl.BlockSpec((image_rows, channels), lambda i: (i, 0)),
            pl.BlockSpec((1, height, width, channels), lambda i: (i, 0, 0, 0)),
            whole(blocks, LANES, LANES),
            whole(blocks, LANES, LANES),
            whole(1, channels),
            whole(1, channels),
        ],
        out_specs=pl.BlockSpec((1, height, width, channels), lambda i: (i, 0, 0, 0)),
        scratch_shapes=[pltpu.VMEM((image_rows, channels), BF16)],
        compiler_params=pltpu.CompilerParams(vmem_limit_bytes=VMEM_LIMIT),
        name="final",
    )(back, features, w_pairs, s_pairs, (back_total / pixel_total)[None], channel_mean[None])

    index = lax.axis_index("batch") * shape[1] + lax.axis_index("rows")
    whitened_mean = jnp.einsum(
        "gj,gji->gi",
        channel_mean.reshape(groups, group_size),
        whiten.astype(BF16).astype(F32),
        precision=highest,
    ).reshape(channels)
    mine = lax.dynamic_slice(whitened_mean, (index * per,), (per,))
    grad = share - colsum[:, None, :] * mine[None, :, None]
    kernel_grad = grad.transpose(1, 0, 2).reshape(per, 3, 3, outputs)
    return (input_grad, kernel_grad)


def solution(mesh):
    shape = (mesh.shape["batch"], mesh.shape["rows"])
    split = P(("batch", "rows"), None, None, None)
    return jax.shard_map(
        functools.partial(local, shape),
        mesh=mesh,
        in_specs=(split, split, P(), P(), P()),
        out_specs=(split, split),
        check_vma=False,
    )
```

```python
import functools
import jax
import jax.numpy as jnp
from jax import lax
from jax.experimental import pallas as pl
from jax.experimental.pallas import tpu as pltpu
from jax.sharding import PartitionSpec as P

highest = lax.Precision.HIGHEST
F32, BF16 = jnp.float32, jnp.bfloat16
LANES = 128
VMEM_LIMIT = 63 * 1024 * 1024


def round_up(n, m):
    return (n + m - 1) // m * m


def bit_orders(bits):
    rest = list(range(1, bits))
    first = [0] + rest
    second = [0] + rest[1:2] + rest[:1] + rest[2:]
    third = [0] + rest[2:3] + rest[:2] + rest[3:]
    return [first, second, third]


def slot_of(index, order):
    slot = 0
    count = len(order)
    for step, bit in enumerate(order):
        slot = slot + (index // 2**bit) % 2 * 2 ** (count - 1 - step)
    return slot


def step_kernel(
    sizes, f_ref, g_ref, k_hbm, v_ref, sv_ref, o_ref, share_ref,
    fp, ft, cols, gpad, k_ref, back, w_ref, s_ref, flat, small, total, column, pieces,
    k_sem, send_sem, recv_sem, *scratch
):
    (nb, nr, images, height, width, wide, channels, outputs, per, orders, streams, pixel_total) = sizes
    rows = images * height * wide
    kp = fp.shape[0]
    blocks = channels // LANES
    taps = 3 * outputs
    part_width = 3 * taps // streams
    bits = len(orders[0])
    count = 2**bits
    rp = small.shape[1]
    half = LANES // 2
    base = channels // 2
    image_rows = height * wide
    batch = lax.axis_index("batch")
    row = lax.axis_index("rows")
    index = batch * nr + row

    def bit_of(bit):
        return (index // 2**bit) % 2

    def partner(bit):
        sign = 1 - 2 * bit_of(bit)
        if 2**bit < nr:
            return (batch, row + sign * 2**bit)
        return (batch + sign * (2**bit // nr), row)

    barrier = pltpu.get_barrier_semaphore()
    for bit in range(bits):
        pl.semaphore_signal(
            barrier, inc=1, device_id=partner(bit), device_id_type=pl.DeviceIdType.MESH
        )
    k_copy = pltpu.make_async_copy(k_hbm, k_ref, k_sem)
    k_copy.start()

    fp[pl.ds(rows, kp - rows), :] = jnp.zeros((kp - rows, channels), BF16)
    cols[pl.ds(rows, kp - rows), :] = jnp.zeros((kp - rows, 3 * taps), BF16)
    gpad[...] = jnp.zeros(gpad.shape, F32)

    @pl.loop(0, images)
    def _(b):
        gpad[pl.ds(1, height), pl.ds(1, width), :] = g_ref[b].astype(F32)
        for h in range(height):
            at = pl.multiple_of((b * height + h) * wide, 16)
            fp[pl.ds(at, wide), :] = jnp.zeros((wide, channels), BF16)
            fp[pl.ds(at, width), :] = f_ref[b, h]
        at = pl.multiple_of(b * image_rows, 16)
        for c in range(3):
            shifted = gpad[:, 2 - c : 2 - c + wide, :].astype(BF16)
            for a in range(3):
                first = a * taps + c * outputs
                cols[pl.ds(at, image_rows), first : first + outputs] = shifted[
                    2 - a : 2 - a + height
                ].reshape(image_rows, outputs)

    @pl.loop(0, blocks)
    def _(k):
        at = pl.ds(pl.multiple_of(k * LANES, LANES), LANES)
        ft[at, :] = fp[:, at].T
        v = v_ref[k]
        w_ref[k] = lax.dot_general(
            v * sv_ref[0, pl.ds(k, 1), :], v, (((1,), (1,)), ((), ())),
            precision=highest, preferred_element_type=F32,
        ).astype(BF16)

    position = lax.broadcasted_iota(jnp.int32, (kp, 1), 0)
    valid = (position % wide < width) & (position < rows)
    lane = lax.broadcasted_iota(jnp.int32, (8, kp), 1)
    ones = jnp.where((lane % wide < width) & (lane < rows), 1.0, 0.0).astype(BF16)
    low_lane = lax.broadcasted_iota(jnp.int32, (half, LANES), 1) < half
    flat[pl.ds(base, flat.shape[0] - base), :] = jnp.zeros((flat.shape[0] - base, LANES), F32)

    step = 2 * LANES
    k_copy.wait()

    @pl.loop(0, channels // step)
    def _(n):
        at = pl.ds(pl.multiple_of(n * step, step), step)
        grad = jnp.dot(cols[...], k_ref[:, at], preferred_element_type=F32)
        back[:, at] = grad
        summed = jnp.sum(jnp.where(valid, grad, 0.0), axis=0, keepdims=True)
        low = grad.astype(BF16)
        raw = jnp.dot(ft[at, :], low, preferred_element_type=F32)
        fsum = jnp.dot(ones, fp[:, at], preferred_element_type=F32)
        for q in range(2):
            block = raw[q * LANES : (q + 1) * LANES, q * LANES : (q + 1) * LANES]
            where = pl.multiple_of((2 * n + q) * half, half)
            flat[pl.ds(where, half), :] = jnp.where(low_lane, block[:half], block[half:])
            flat[pl.ds(base + 2 * n + q, 1), :] = summed[:, q * LANES : (q + 1) * LANES]
            flat[pl.ds(base + blocks + 2 * n + q, 1), :] = fsum[:1, q * LANES : (q + 1) * LANES]

    colsum = jnp.dot(ones, cols[...], preferred_element_type=F32)
    for q in range(3 * taps // LANES):
        flat[pl.ds(base + 2 * blocks + q, 1), :] = colsum[:1, q * LANES : (q + 1) * LANES]

    @pl.loop(0, count)
    def _(i):
        small[i] = flat[pl.ds(pl.multiple_of(i * rp, 8), rp), :]

    def copy(src, dst, s, t, bit):
        c = pltpu.make_async_remote_copy(
            src_ref=src,
            dst_ref=dst,
            send_sem=send_sem.at[s, t],
            recv_sem=recv_sem.at[s, t],
            device_id=partner(bit),
            device_id_type=pl.DeviceIdType.MESH,
        )
        c.start()
        return c

    sources = [pieces.at[s] for s in range(streams)] + [small]
    buffers = [[scratch[s * bits + t] for t in range(bits)] for s in range(streams + 1)]
    all_orders = [orders[s % 3] for s in range(streams)] + [orders[0]]
    flights = {}

    def begin(s, t):
        bit = all_orders[s][t]
        size = count >> (t + 1)
        src = sources[s] if t == 0 else buffers[s][t - 1]
        flights[s] = copy(
            src.at[pl.ds((1 - bit_of(bit)) * size, size)], buffers[s][t], s, t, bit
        )

    def finish(s, t):
        size = count >> (t + 1)
        src = sources[s] if t == 0 else buffers[s][t - 1]
        dst = buffers[s][t]
        flights[s].wait()
        first = bit_of(all_orders[s][t]) * size

        @pl.loop(0, size)
        def _(i):
            dst[i] = dst[i] + src[first + i]

    slot = slot_of(index, all_orders[streams])

    def spread(u):
        region = pl.ds(slot // 2**u * 2**u, 2**u)
        flights[streams] = copy(
            total.at[region], total.at[region], streams, bits + u,
            all_orders[streams][bits - 1 - u],
        )

    def advance(t):
        if t < bits:
            finish(streams, t)
            if t + 1 < bits:
                begin(streams, t + 1)
            else:
                total[slot] = buffers[streams][t][0]
                spread(0)
        else:
            flights[streams].wait()
            if t + 1 < 2 * bits:
                spread(t + 1 - bits)

    def piece(s):
        high = 4 * LANES

        @pl.loop(0, channels // high)
        def _(m):
            at = pl.ds(pl.multiple_of(m * high, high), high)
            part = jnp.dot(
                ft[at, :],
                cols[:, s * part_width : (s + 1) * part_width],
                preferred_element_type=F32,
            )
            for q in range(4):
                weight = w_ref[4 * m + q]
                block = part[q * LANES : (q + 1) * LANES]
                one = block.astype(BF16)
                left = block - one.astype(F32)
                two = left.astype(BF16)
                three = (left - two.astype(F32)).astype(BF16)
                result = sum(
                    lax.dot_general(
                        weight, x, (((0,), (0,)), ((), ())), preferred_element_type=F32
                    )
                    for x in (one, two, three)
                )
                for j in range(LANES // per):
                    chunk = (4 * m + q) * (LANES // per) + j
                    pieces[s, slot_of(chunk, all_orders[s])] = result[j * per : (j + 1) * per]

    pl.semaphore_wait(barrier, bits)
    begin(streams, 0)
    done = 0
    for s in range(streams):
        piece(s)
        begin(s, 0)
        if s > 0:
            finish(s - 1, 0)
            begin(s - 1, 1)
        if done < 2 * bits:
            advance(done)
            done += 1
    finish(streams - 1, 0)
    begin(streams - 1, 1)
    for s in range(streams):
        if done < 2 * bits:
            advance(done)
            done += 1
        finish(s, 1)
        begin(s, 2)
    while done < 2 * bits:
        advance(done)
        done += 1

    @pl.loop(0, count)
    def _(i):
        flat[pl.ds(pl.multiple_of(i * rp, 8), rp), :] = total[i]

    def across(line):
        return jnp.broadcast_to(line, (LANES, LANES)).T

    side = lax.broadcasted_iota(jnp.int32, (LANES, LANES), 0) < half
    other = lax.broadcasted_iota(jnp.int32, (LANES, LANES), 1) < half
    inside = side == other

    @pl.loop(0, blocks)
    def _(k):
        packed = flat[pl.ds(pl.multiple_of(k * half, half), half), :]
        mean = flat[pl.ds(base + blocks + k, 1), :] / pixel_total
        summed = flat[pl.ds(base + k, 1), :]
        raw = jnp.concatenate([packed, packed], axis=0)
        cov = jnp.where(inside, raw - across(mean) * summed, 0.0)
        v = v_ref[k]
        scale = sv_ref[0, pl.ds(k, 1), :]
        root = sv_ref[1, pl.ds(k, 1), :]
        turned = lax.dot_general(
            v, cov, (((0,), (0,)), ((), ())), precision=highest, preferred_element_type=F32
        )
        rotated = jnp.dot(turned, v, precision=highest, preferred_element_type=F32)
        symmetric = 0.5 * (rotated + rotated.T)
        factor = -(across(scale) * scale) / (across(root) + root)
        inner = jnp.where(inside, symmetric * factor, 0.0)
        outer = jnp.dot(v, inner, precision=highest, preferred_element_type=F32)
        sigma = lax.dot_general(
            outer, v, (((1,), (1,)), ((), ())), precision=highest, preferred_element_type=F32
        )
        s_ref[k] = (2.0 / pixel_total * sigma).astype(BF16)

    @pl.loop(0, images)
    def _(b):
        here = pl.ds(pl.multiple_of(b * image_rows, 16), image_rows)
        for k in range(blocks):
            at = slice(k * LANES, (k + 1) * LANES)
            mean = flat[base + blocks + k : base + blocks + k + 1, :] / pixel_total
            shift = flat[base + k : base + k + 1, :] / pixel_total
            shifted = (back[here, at] - shift).astype(BF16)
            centered = (fp[here, at].astype(F32) - mean).astype(BF16)
            out = jnp.dot(shifted, w_ref[k], preferred_element_type=F32) + jnp.dot(
                centered, s_ref[k], preferred_element_type=F32
            )
            o_ref[b, :, :, at] = out.astype(BF16).reshape(height, wide, LANES)[:, :width]

    for t in range(2, bits):
        for s in range(streams):
            finish(s, t)
            if t + 1 < bits:
                begin(s, t + 1)

    mine = index * per // LANES
    mean = flat[pl.ds(base + blocks + mine, 1), :] / pixel_total
    whitened = jnp.dot(
        jnp.broadcast_to(mean, (8, LANES)), w_ref[mine].astype(F32),
        precision=highest, preferred_element_type=F32,
    )
    column[...] = across(whitened[:1])
    mean_part = column[pl.ds(pl.multiple_of(index * per % LANES, per), per), :]
    for s in range(streams):
        for q in range(part_width // LANES):
            at = s * (part_width // LANES) + q
            line = flat[base + 2 * blocks + at : base + 2 * blocks + at + 1, :]
            share_ref[:, at * LANES : (at + 1) * LANES] = (
                buffers[s][bits - 1][0, :, q * LANES : (q + 1) * LANES] - mean_part * line
            )


def pair_blocks(blocks):
    groups, size = blocks.shape[:2]
    pairs = blocks.reshape(groups // 2, 2, size, size)
    zero = jnp.zeros((groups // 2, size, size), blocks.dtype)
    top = jnp.concatenate([pairs[:, 0], zero], axis=2)
    bottom = jnp.concatenate([zero, pairs[:, 1]], axis=2)
    return jnp.concatenate([top, bottom], axis=1)


def local(shape, features, grads, kernel, vectors, values):
    images, height, width, channels = features.shape
    outputs = grads.shape[3]
    groups, group_size = values.shape
    devices = shape[0] * shape[1]
    bits = devices.bit_length() - 1
    orders = bit_orders(bits)
    per = channels // devices
    taps = 3 * outputs
    wide = round_up(width, 16)
    rows = images * height * wide
    kp = round_up(rows + 1, LANES)
    blocks = channels // LANES
    pixel_total = 1.0 * images * height * width * devices
    small_rows = channels // 2 + 2 * blocks + 3 * taps // LANES
    rp = round_up(-(-small_rows // devices), 8)

    streams = 6
    part_width = 3 * taps // streams
    lines = jnp.stack([lax.rsqrt(values), jnp.sqrt(values)]).reshape(2, blocks, LANES)
    vmem = pl.BlockSpec(memory_space=pltpu.VMEM)
    scratch = []
    for _ in range(streams):
        scratch += [pltpu.VMEM((devices >> (t + 1), per, part_width), F32) for t in range(bits)]
    scratch += [pltpu.VMEM((devices >> (t + 1), rp, LANES), F32) for t in range(bits)]
    sizes = (
        shape[0], shape[1], images, height, width, wide, channels, outputs, per, orders,
        streams, pixel_total,
    )
    input_grad, share = pl.pallas_call(
        functools.partial(step_kernel, sizes),
        out_shape=(
            jax.ShapeDtypeStruct(features.shape, BF16),
            jax.ShapeDtypeStruct((per, 3 * taps), F32),
        ),
        in_specs=[vmem, vmem, pl.BlockSpec(memory_space=pl.ANY), vmem, vmem],
        out_specs=(vmem, vmem),
        scratch_shapes=[
            pltpu.VMEM((kp, channels), BF16),
            pltpu.VMEM((channels, kp), BF16),
            pltpu.VMEM((kp, 3 * taps), BF16),
            pltpu.VMEM((height + 2, wide + 8, outputs), F32),
            pltpu.VMEM((3 * taps, channels), BF16),
            pltpu.VMEM((kp, channels), F32),
            pltpu.VMEM((blocks, LANES, LANES), BF16),
            pltpu.VMEM((blocks, LANES, LANES), BF16),
            pltpu.VMEM((devices * rp, LANES), F32),
            pltpu.VMEM((devices, rp, LANES), F32),
            pltpu.VMEM((devices, rp, LANES), F32),
            pltpu.VMEM((LANES, LANES), F32),
            pltpu.VMEM((streams, devices, per, part_width), F32),
            pltpu.SemaphoreType.DMA,
            pltpu.SemaphoreType.DMA((streams + 1, 2 * bits)),
            pltpu.SemaphoreType.DMA((streams + 1, 2 * bits)),
        ]
        + scratch,
        compiler_params=pltpu.CompilerParams(
            collective_id=0, has_side_effects=True, vmem_limit_bytes=VMEM_LIMIT
        ),
        name="step",
    )(features, grads, kernel.reshape(3 * taps, channels), pair_blocks(vectors), lines)
    return (input_grad, share.reshape(per, 3, 3, outputs))


def solution(mesh):
    shape = (mesh.shape["batch"], mesh.shape["rows"])
    split = P(("batch", "rows"), None, None, None)
    return jax.shard_map(
        functools.partial(local, shape),
        mesh=mesh,
        in_specs=(split, split, P(), P(), P()),
        out_specs=(split, split),
        check_vma=False,
    )
```
